512 devices in a mesh: dp: 64 (over x, y, core), head: 8 (over z).
Axes of the slice: x: 4, y: 8, z: 8, core: 2. Of those that a mesh axis runs over, the one named last changes fastest.
Arguments:
- features: bfloat16 [2, 512, 196, 1024], P(None, ('dp', 'head'))
- patch_mask: int32 [2, 512, 196], P(None, ('dp', 'head')), may hold values from 0 to 1, as said below
- w_first: bfloat16 [1024, 2048], P('dp'), may hold values from -0.1875 to 0.1875
- w_second: bfloat16 [2048, 256], P('dp'), may hold values from -0.125 to 0.125
- proto_weight: bfloat16 [256, 8192], P('dp', 'head'), may hold values from -6 to 6
- center: float32 [8192], replicated, may hold values from -0.04 to 0.04
Outputs:
- targets: bfloat16 [2, 50176, 8192], P(None, ('dp', 'head'))
- new_center: float32 [8192], P('head')
The draws below stay inside these ranges and needn't reach their ends.
Inputs may be any that keep to these rules, and one draw needn't show every extreme that they name: `patch_mask`: in each view every image masks between 19 and 98 of its patches, so that a block of 1 images fills at most 98 slots; in every draw the images of some block fill all 98 slots.
All inputs are finite; a program needn't handle non-finite values.
Results may differ from the reference program's by a relative error of at most 0.0086.
Values may be sent and summed in bfloat16 or wider, within the bound.
A program may use at most 64 MiB of HBM per device.

```python
import jax
import jax.numpy as jnp
from jax import lax

D = 1024
HID = 2048
BOT = 256
PROTO = 8192
PATCH = 196
VIEWS = 2
IMG_DEV = 1
MAXMASK = 98
CAP = 98
IMAGES = 512
SLOTS = 50176
N_DP = 64
N_HEAD = 8


def draw_features(key, part):
    key = jax.random.fold_in(key, 11)
    k_noise, k_first, k_second = jax.random.split(key, 3)
    shape = (VIEWS, IMAGES, PATCH, D)
    along = (jnp.arange(IMAGES, dtype=jnp.float32) / IMAGES).reshape(1, IMAGES, 1, 1)
    first = jax.random.normal(k_first, (VIEWS, 1, 1, D), jnp.float32)
    second = jax.random.normal(k_second, (VIEWS, 1, 1, D), jnp.float32)
    noise = jax.random.normal(k_noise, shape, jnp.float32)
    values = noise + 0.7 * first + 1.4 * along * second
    return values.astype(jnp.bfloat16)


def draw_patch_mask(key, part):
    key = jax.random.fold_in(key, 23)
    k_count, k_order, k_full = jax.random.split(key, 3)
    image = jnp.arange(IMAGES, dtype=jnp.int32)
    lowest = PATCH // 10 + PATCH * 4 // 10 * image // IMAGES
    counts = jax.random.randint(k_count, (VIEWS, IMAGES), 0, PATCH // 10 + 1, dtype=jnp.int32) + lowest[None, :]
    counts = jnp.minimum(counts, MAXMASK)
    full_block = jax.random.randint(k_full, (), 0, IMAGES // IMG_DEV, dtype=jnp.int32)
    counts = jnp.where((image // IMG_DEV == full_block)[None, :], MAXMASK, counts)
    scores = jax.random.randint(k_order, (VIEWS, IMAGES, PATCH), 0, 1 << 20, dtype=jnp.int32) * PATCH + jnp.arange(PATCH, dtype=jnp.int32)
    ranks = jnp.argsort(jnp.argsort(scores, axis=-1, stable=True), axis=-1, stable=True).astype(jnp.int32)
    return (ranks < counts[:, :, None]).astype(jnp.int32)


def levels(own_key, extent, cuts, smallest, top_value):
    factor_of, own = 1.0, jax.random.fold_in(own_key, 6)
    for axis_at, blocks in cuts:
        heights = jnp.exp(jax.random.uniform(jax.random.fold_in(own, axis_at), (blocks,), jnp.float32, smallest / len(cuts), top_value / len(cuts)))
        factor_of = factor_of * jnp.repeat(heights, extent[axis_at] // blocks).reshape([-1 if axis == axis_at else 1 for axis in range(len(extent))])
    return factor_of


def bell_draw(stream_key, extent, scale, reach, shards=(), kind=jnp.bfloat16):
    loudness = levels(stream_key, extent, shards, -0.22, 0.18) if shards else 1.0
    array = jax.random.normal(stream_key, extent, jnp.float32) * scale * loudness
    return jnp.minimum(jnp.maximum(array, -reach), reach).astype(kind)


def setup_inputs(seed: int = 0) -> dict:
    key_list = jax.random.split(jax.random.key(seed), 7)
    features = draw_features(jax.random.fold_in(key_list[6], 71), 0)
    patch_mask = draw_patch_mask(jax.random.fold_in(key_list[6], 71), 0)
    w_first = bell_draw(key_list[2], (D, HID), D ** -0.5, 0.1875, ((0, 64),))
    w_second = bell_draw(key_list[3], (HID, BOT), HID ** -0.5, 0.125, ((0, 64),))
    proto_weight = bell_draw(key_list[4], (BOT, PROTO), 1.0, 6.0, ((0, 64), (1, 8)))
    center = bell_draw(key_list[5], (PROTO,), 0.01, 0.04, (), jnp.float32)
    return dict(features=features, patch_mask=patch_mask, w_first=w_first, w_second=w_second, proto_weight=proto_weight, center=center)


teacher_temp = 0.04
center_momentum = 0.9

def pack_block(block_feats, block_mask):
    flat_mask = block_mask.reshape(-1)
    flat_feats = block_feats.reshape(-1, block_feats.shape[-1])
    places = jnp.nonzero(flat_mask, size=CAP, fill_value=0)[0].astype(jnp.int32)
    live = jnp.arange(CAP, dtype=jnp.int32) < jnp.sum(flat_mask).astype(jnp.int32)
    rows = jnp.where(live[:, None], flat_feats[places], jnp.zeros((), flat_feats.dtype))
    return (rows, live)

def bottleneck(rows, w_first, w_second):
    hidden = jax.nn.gelu(jnp.dot(rows, w_first, preferred_element_type=jnp.float32), approximate=False).astype(jnp.bfloat16)
    projected = jnp.dot(hidden, w_second, preferred_element_type=jnp.float32)
    scale = lax.rsqrt(lax.optimization_barrier(jnp.sum(projected * projected, axis=-1, keepdims=True)) + 1e-06)
    return (projected * scale).astype(jnp.bfloat16)

def reference(features, patch_mask, w_first, w_second, proto_weight, center):
    blocks = N_DP * N_HEAD
    feats = features.reshape(VIEWS, blocks, IMG_DEV * PATCH, D)
    masks = patch_mask.reshape(VIEWS, blocks, IMG_DEV * PATCH)
    columns = proto_weight.astype(jnp.float32)
    unit_protos = (columns * lax.rsqrt(lax.optimization_barrier(jnp.sum(columns * columns, axis=0, keepdims=True)) + 1e-06)).astype(jnp.bfloat16)
    outputs = []
    current = center
    for view in range(VIEWS):

        def one_block(pair, current=current):
            rows, live = pack_block(pair[0], pair[1])
            normed = bottleneck(rows, w_first, w_second)
            logits = jnp.dot(normed, unit_protos, preferred_element_type=jnp.float32)
            exps = jnp.exp((logits - current) / teacher_temp)
            probs = PROTO * exps / lax.optimization_barrier(jnp.sum(exps, axis=1, keepdims=True))
            targets = jnp.where(live[:, None], probs, jnp.zeros((), jnp.float32)).astype(jnp.bfloat16)
            return (targets, lax.optimization_barrier(jnp.sum(logits, axis=0)), jnp.sum(live.astype(jnp.float32)))
        targets, partials, counts = lax.map(one_block, (feats[view], masks[view]))
        outputs.append(targets.reshape(SLOTS, PROTO))
        current = center_momentum * current + (1.0 - center_momentum) * lax.optimization_barrier(jnp.sum(partials, axis=0)) / jnp.sum(counts)
    return (jnp.stack(outputs), current)
```

```python
import functools

import jax
import jax.numpy as jnp
from jax import lax
from jax.experimental import pallas as pl
from jax.experimental.pallas import tpu as pltpu
from jax.sharding import PartitionSpec as P

MESH = pl.DeviceIdType.MESH
ANY = pl.BlockSpec(memory_space=pl.ANY)
VM = pl.BlockSpec(memory_space=pltpu.VMEM)

teacher_temp = 0.04
center_momentum = 0.9

NX, NY, NZ = 4, 8, 8
VIEWS, PATCH, CAP, PADCAP = 2, 196, 98, 104
D, HID, BOT, PROTO = 1024, 2048, 256, 8192
SHARE = PROTO // NZ
ACOLS = 1024
WCOLS = HID + 2 * BOT
F32 = jnp.float32
BF16 = jnp.bfloat16


def place():
    dp = lax.axis_index("dp")
    z = lax.axis_index("head")
    return dp // (2 * NY), (dp // 2) % NY, dp % 2, z


def dp_of(x, y, c):
    return (x * NY + y) * 2 + c


Y_ORDER = (0, 1, 7, 2, 6, 3, 5, 4)
RIGHT_HALF = (0, 7, 2, 5)


def plan():
    events = []
    for d, t in ((1, 2.6), (3, 2.7), (2, 3.3)):
        events.append((t, "ax", 0, d, 0))
    avail = {0: 0.0}
    for k in range(1, 5):
        for side in (0, 1):
            events.append((3.0 + 2.6 * (k - 1) + 0.01 * side, "by", side, k, 0))
            events.append((4.6 + 2.6 * (k - 1) + 0.01 * side, "py", side, k, 0))
        avail[k] = avail[8 - k] = 3.0 + 2.6 * (k - 1)
    pavail = {0: 2.2}
    for k in range(1, 5):
        pavail[k] = pavail[8 - k] = 4.6 + 2.6 * (k - 1)
    start = {0: 0.0, 1: 2.6, 3: 2.7, 2: 3.3}
    clock = 3.0
    for k in range(1, 5):
        for side in (0, 1):
            for i, j in enumerate((0, 1, 3, 2)):
                if k == 4 and (j in (0, 1)) != (side == 0):
                    continue
                t = max(start[j] + 2.4 * k, 3.4 + 3.0 * (k - 1) + 0.75 * i)
                events.append((t + 0.01 * side, "ay", side, k, j))
    for k in (1, 2):
        for side in (0, 1):
            for i, d in enumerate(Y_ORDER):
                if k == 2 and (d in RIGHT_HALF) != (side == 0):
                    continue
                if k == 1:
                    t = max(avail[d] + 2.2, 2.5 + 1.2 * i)
                else:
                    t = max(avail[d] + 4.4, 12.0 + 0.6 * i)
                events.append((t + 0.01 * side, "bx", side, k, d))
    for k in range(1, 5):
        for side in (0, 1):
            for i, d in enumerate(Y_ORDER):
                if k == 4 and (d in RIGHT_HALF) != (side == 0):
                    continue
                t = max(pavail[d] + 2.0 * k, 4.5 + 5.6 * (k - 1) + 0.7 * i)
                events.append((t + 0.01 * side, "pz", side, k, d))
    return sorted(events)


EVENTS = plan()


def gather_kernel(w1, w2, pw, wbuf, pbuf, px, lsem, px_s, px_r, ax_s, ax_r,
                  by_s, by_r, py_s, py_r, ay_s, ay_r, bx_s, bx_r, pz_s, pz_r, dd_s, dd_r):
    x, y, c, z = place()

    def at_x(n):
        return lax.rem(x + n + NX, NX)

    def at_y(n):
        return lax.rem(y + n + NY, NY)

    def at_z(n):
        return lax.rem(z + n + NZ, NZ)

    def dev(nx=0, ny=0, nz=0, other=False):
        return (dp_of(at_x(nx), at_y(ny), 1 - c if other else c), at_z(nz))

    cols_a, cols_b = pl.ds(0, ACOLS), pl.ds(ACOLS, WCOLS - ACOLS)
    loads = [
        pltpu.make_async_copy(pw, px.at[x], lsem.at[0]),
        pltpu.make_async_copy(w1, wbuf.at[x, y, c, :, pl.ds(0, HID)], lsem.at[1]),
        pltpu.make_async_copy(w2.at[pl.ds(0, 16)], wbuf.at[x, y, c, :, pl.ds(HID, BOT)], lsem.at[2]),
        pltpu.make_async_copy(w2.at[pl.ds(16, 16)], wbuf.at[x, y, c, :, pl.ds(HID + BOT, BOT)], lsem.at[3]),
    ]
    for copy in loads:
        copy.start()
    peers = [dev(nx=n) for n in (1, 2, 3)] + [dev(ny=1), dev(ny=-1), dev(nz=1), dev(nz=-1), dev(other=True)]
    barrier = pltpu.get_barrier_semaphore()
    for peer in peers:
        pl.semaphore_signal(barrier, inc=1, device_id=peer, device_id_type=MESH)
    pl.semaphore_wait(barrier, len(peers))
    for copy in loads:
        copy.wait()

    sent = []

    def send(ref, s, r, to):
        copy = pltpu.make_async_remote_copy(
            src_ref=ref, dst_ref=ref, send_sem=s, recv_sem=r, device_id=to, device_id_type=MESH
        )
        copy.start()
        sent.append(copy)

    def landed(ref, s, r, to):
        pltpu.make_async_remote_copy(
            src_ref=ref, dst_ref=ref, send_sem=s, recv_sem=r, device_id=to, device_id_type=MESH
        ).wait_recv()

    def half(cols, side):
        start, size = cols
        return pl.ds(start + side * (size // 2), size // 2)

    BALL, PALL = (ACOLS, WCOLS - ACOLS), (0, SHARE)

    def a_ref(nx, ny):
        return wbuf.at[at_x(nx), at_y(ny), c, :, cols_a]

    def b_ref(nx, ny, side=None):
        cols = cols_b if side is None else half(BALL, side)
        return wbuf.at[at_x(nx), at_y(ny), c, :, cols]

    def p_ref(nz, ny, side=None):
        cols = pl.ds(*PALL) if side is None else half(PALL, side)
        return pbuf.at[at_z(nz), c, at_y(ny), :, cols]

    def sgn(side):
        return 1 if side == 0 else -1

    def back(side, k):
        return -k * sgn(side)

    counts = {}
    for g in range(NY):
        counts["a", g] = 4
        counts["p", g] = 8
    for g in range(NX):
        counts["b", g] = 8
    counts["b", 0] = 9
    counts["p", 0] = 9
    counts["b", 2], counts["p", 4] = 8, 8

    def done(kind, g):
        counts[kind, g] -= 1
        if counts[kind, g]:
            return
        to = dev(other=True)
        if kind == "a":
            send(wbuf.at[:, at_y(-g), c, :, cols_a], dd_s.at[g], dd_r.at[g], to)
        elif kind == "b":
            send(wbuf.at[at_x(-g), :, c, :, cols_b], dd_s.at[8 + g], dd_r.at[8 + g], to)
        else:
            send(pbuf.at[at_z(-g), c], dd_s.at[12 + g], dd_r.at[12 + g], to)

    def forward_by(side, k):
        if k <= 3:
            send(b_ref(0, back(side, k - 1)), by_s.at[side, k - 1], by_r.at[side, k - 1], dev(ny=sgn(side)))
        else:
            send(b_ref(0, back(side, 3), side), by_s.at[side, 3], by_r.at[side, 3], dev(ny=sgn(side)))

    def forward_py(side, k):
        if k <= 3:
            send(p_ref(0, back(side, k - 1)), py_s.at[side, k - 1], py_r.at[side, k - 1], dev(ny=sgn(side)))
        else:
            send(p_ref(0, back(side, 3), side), py_s.at[side, 3], py_r.at[side, 3], dev(ny=sgn(side)))

    def forward_ay(side, k, j):
        if k == 4 and (j in (0, 1)) != (side == 0):
            return
        send(a_ref(-j, back(side, k - 1)), ay_s.at[side, k - 1, j], ay_r.at[side, k - 1, j], dev(ny=sgn(side)))

    def forward_bx(side, k, d):
        if k == 2 and (d in RIGHT_HALF) != (side == 0):
            return
        send(b_ref(back(side, k - 1), -d), bx_s.at[side, k - 1, d], bx_r.at[side, k - 1, d], dev(nx=sgn(side)))

    def forward_pz(side, k, d):
        if k == 4 and (d in RIGHT_HALF) != (side == 0):
            return
        send(p_ref(back(side, k - 1), -d), pz_s.at[side, k - 1, d], pz_r.at[side, k - 1, d], dev(nz=sgn(side)))

    for n in (1, 3, 2):
        send(px.at[x], px_s.at[n], px_r.at[n], dev(nx=n))
    for n in (1, 3, 2):
        send(a_ref(0, 0), ax_s.at[n], ax_r.at[n], dev(nx=n))
    for side in (0, 1):
        forward_by(side, 1)
    for side in (0, 1):
        forward_bx(side, 1, 0)
        forward_ay(side, 1, 0)
    done("a", 0)
    done("b", 0)

    for n in (1, 3, 2):
        landed(px.at[at_x(-n)], px_s.at[n], px_r.at[n], dev(nx=n))
    pbuf[z, c, y] = px[...].reshape(16, SHARE)
    early = [e for e in EVENTS if e[1] in ("ax", "by") and e[0] < 3.2]
    late = [e for e in EVENTS if e not in early]

    def handle(event):
        _, stream, side, k, j = event
        if stream == "ax":
            landed(a_ref(-k, 0), ax_s.at[k], ax_r.at[k], dev(nx=k))
            for s in (0, 1):
                forward_ay(s, 1, k)
            done("a", 0)
        elif stream == "by":
            ref = b_ref(0, back(side, k), None if k < 4 else side)
            landed(ref, by_s.at[side, k - 1], by_r.at[side, k - 1], dev(ny=1))
            if k < 4:
                forward_by(side, k + 1)
            counts["y4"] = counts.get("y4", 0) + (k == 4)
            if k < 4 or counts["y4"] == 2:
                for s in (0, 1):
                    forward_bx(s, 1, k if side == 0 else 8 - k) if k < 4 else forward_bx(s, 1, 4)
            done("b", 0)
        elif stream == "py":
            ref = p_ref(0, back(side, k), None if k < 4 else side)
            landed(ref, py_s.at[side, k - 1], py_r.at[side, k - 1], dev(ny=1))
            if k < 4:
                forward_py(side, k + 1)
            counts["p4"] = counts.get("p4", 0) + (k == 4)
            if k < 4 or counts["p4"] == 2:
                for s in (0, 1):
                    forward_pz(s, 1, k if side == 0 else 8 - k) if k < 4 else forward_pz(s, 1, 4)
            done("p", 0)
        elif stream == "ay":
            landed(a_ref(-j, back(side, k)), ay_s.at[side, k - 1, j], ay_r.at[side, k - 1, j], dev(ny=1))
            if k < 4:
                forward_ay(side, k + 1, j)
            done("a", k if side == 0 else 8 - k)
        elif stream == "bx":
            landed(b_ref(back(side, k), -j), bx_s.at[side, k - 1, j], bx_r.at[side, k - 1, j], dev(nx=1))
            if k < 2:
                forward_bx(side, k + 1, j)
            done("b", k if side == 0 else 4 - k)
        else:
            landed(p_ref(back(side, k), -j), pz_s.at[side, k - 1, j], pz_r.at[side, k - 1, j], dev(nz=1))
            if k < 4:
                forward_pz(side, k + 1, j)
            done("p", k if side == 0 else 8 - k)

    for event in early:
        handle(event)
    for side in (0, 1):
        forward_py(side, 1)
        forward_pz(side, 1, 0)
    done("p", 0)
    for event in late:
        handle(event)

    assert not any(v for k, v in counts.items() if isinstance(k, tuple)), counts
    other = 1 - c
    for g in range(8):
        landed(wbuf.at[:, at_y(-g), other, :, cols_a], dd_s.at[g], dd_r.at[g], dev(other=True))
        landed(pbuf.at[at_z(-g), other], dd_s.at[12 + g], dd_r.at[12 + g], dev(other=True))
    for g in range(4):
        landed(wbuf.at[at_x(-g), :, other, :, cols_b], dd_s.at[8 + g], dd_r.at[8 + g], dev(other=True))
    for copy in sent:
        copy.wait_send()


def gather(w_first, w_second, proto_weight):
    dma = pltpu.SemaphoreType.DMA
    return pl.pallas_call(
        gather_kernel,
        out_shape=(
            jax.ShapeDtypeStruct((NX, NY, 2, 16, WCOLS), BF16),
            jax.ShapeDtypeStruct((NZ, 2, NY, 16, SHARE), BF16),
        ),
        in_specs=[ANY] * 3,
        out_specs=(VM, VM),
        scratch_shapes=[
            pltpu.VMEM((NX, 4, SHARE), BF16),
            dma((4,)),
            dma((4,)), dma((4,)), dma((4,)), dma((4,)),
            dma((2, 4)), dma((2, 4)), dma((2, 4)), dma((2, 4)),
            dma((2, 4, 4)), dma((2, 4, 4)), dma((2, 2, 8)), dma((2, 2, 8)),
            dma((2, 4, 8)), dma((2, 4, 8)), dma((20,)), dma((20,)),
        ],
        compiler_params=pltpu.CompilerParams(
            collective_id=0, has_side_effects=True, vmem_limit_bytes=48 << 20
        ),
        name="gather",
    )(w_first, w_second, proto_weight)


def bottleneck_kernel(feats, mask, w, normed, sums, local, rows, hid):
    live = mask[...].astype(F32)
    counts = jnp.sum(live, axis=1, keepdims=True)
    before = lax.broadcasted_iota(jnp.int32, (PATCH, PATCH), 0) <= lax.broadcasted_iota(jnp.int32, (PATCH, PATCH), 1)
    live8 = jnp.concatenate([live, jnp.zeros((6, PATCH), F32)], axis=0)
    rank = jnp.dot(live8.astype(BF16), before.astype(BF16), preferred_element_type=F32)
    slot = lax.broadcasted_iota(jnp.int32, (PADCAP, PATCH), 0).astype(F32) + 1.0
    for v in range(VIEWS):
        pick = (rank[v : v + 1] == slot) & (live[v : v + 1] > 0.5)
        rows[pl.ds(v * PADCAP, PADCAP)] = jnp.dot(
            pick.astype(F32).astype(BF16), feats[v], preferred_element_type=F32
        ).astype(BF16)
    projected = jnp.zeros((VIEWS * PADCAP, BOT), F32)
    wide = HID // NX
    for t in range(NX):
        left = w[:, :, :, :, pl.ds(t * wide, wide)].reshape(D, wide)
        pre = jnp.dot(rows[...], left, preferred_element_type=F32)
        hidden = (0.5 * pre * (1.0 + lax.erf(pre * 0.5**0.5))).astype(BF16)
        low = w[t, :, :, :, pl.ds(HID, BOT)].reshape(16, 16, BOT)
        high = w[t, :, :, :, pl.ds(HID + BOT, BOT)].reshape(16, 16, BOT)
        right = jnp.stack([low, high], axis=1).reshape(wide, BOT)
        projected += jnp.dot(hidden, right, preferred_element_type=F32)
    scale = lax.rsqrt(jnp.sum(projected * projected, axis=-1, keepdims=True) + 1e-06)
    plain = (projected * scale).astype(BF16)
    to = lax.broadcasted_iota(jnp.int32, (BOT, BOT), 1)
    at = lax.broadcasted_iota(jnp.int32, (BOT, BOT), 0)
    source = ((to // 4) % NX) * 64 + ((to // 16) % NY) * 8 + (to // 128) * 4 + to % 4
    ordered = jnp.dot(plain, (at == source).astype(F32).astype(BF16), preferred_element_type=F32)
    normed[...] = ordered.astype(BF16)
    sums[...] = jnp.concatenate(
        [jnp.sum(ordered[v * PADCAP : (v + 1) * PADCAP], axis=0, keepdims=True) for v in range(VIEWS)]
        + [jnp.broadcast_to(counts, (VIEWS, BOT))],
        axis=0,
    )
    local[...] = jnp.broadcast_to(counts, (VIEWS, 128))


def bottleneck(features, patch_mask, w):
    return pl.pallas_call(
        bottleneck_kernel,
        out_shape=(
            jax.ShapeDtypeStruct((VIEWS * PADCAP, BOT), BF16),
            jax.ShapeDtypeStruct((2 * VIEWS, BOT), F32),
            jax.ShapeDtypeStruct((VIEWS, 128), F32),
        ),
        in_specs=[VM] * 3,
        out_specs=(VM,) * 3,
        scratch_shapes=[pltpu.VMEM((VIEWS * PADCAP, D), BF16), pltpu.VMEM((8, 128), F32)],
        compiler_params=pltpu.CompilerParams(vmem_limit_bytes=48 << 20),
        name="bottleneck",
    )(features, patch_mask, w)


def total_kernel(part, out, own, land, s_sem, r_sem):
    x, y, c, z = place()
    stages = (
        [(dp_of(x, y, c), lax.rem(z + n, NZ)) for n in range(1, 8)],
        [(dp_of(x, lax.rem(y + n, NY), c), z) for n in range(1, 8)],
        [(dp_of(lax.rem(x + n % 4, NX), y, lax.rem(c + n // 4, 2)), z) for n in range(1, 8)],
    )
    barrier = pltpu.get_barrier_semaphore()
    for stage in stages:
        for peer in stage:
            pl.semaphore_signal(barrier, inc=1, device_id=peer, device_id_type=MESH)
    pl.semaphore_wait(barrier, 21)
    own[0] = part[...]
    sent = []
    for i, stage in enumerate(stages):
        for n, peer in enumerate(stage):
            copy = pltpu.make_async_remote_copy(
                src_ref=own.at[i], dst_ref=land.at[i, n], send_sem=s_sem.at[i, n],
                recv_sem=r_sem.at[i, n], device_id=peer, device_id_type=MESH,
            )
            copy.start()
            sent.append(copy)
        total = own[i]
        for n in range(7):
            sent[i * 7 + n].wait_recv()
            total = total + land[i, n]
        if i < 2:
            own[i + 1] = total
        else:
            out[...] = total
    for copy in sent:
        copy.wait_send()


def total(part):
    return pl.pallas_call(
        total_kernel,
        out_shape=jax.ShapeDtypeStruct(part.shape, F32),
        in_specs=[VM],
        out_specs=VM,
        scratch_shapes=[
            pltpu.VMEM((3, *part.shape), F32),
            pltpu.VMEM((3, 7, *part.shape), F32),
            pltpu.SemaphoreType.DMA((3, 7)),
            pltpu.SemaphoreType.DMA((3, 7)),
        ],
        compiler_params=pltpu.CompilerParams(collective_id=1, has_side_effects=True),
        name="total",
    )(part)


def targets_kernel(normed, sums, local, protos, center, out, new_center, lhs, exps, totals):
    phase, j = pl.program_id(0), pl.program_id(1)
    z = lax.axis_index("head")
    rows = VIEWS * PADCAP

    @pl.when(phase == 0)
    def _():
        @pl.when(j == 0)
        def _():
            lhs[pl.ds(0, rows)] = normed[...]
            whole = sums[pl.ds(0, VIEWS)]
            high = whole.astype(BF16)
            rest = whole - high.astype(F32)
            mid = rest.astype(BF16)
            low = (rest - mid.astype(F32)).astype(BF16)
            lhs[pl.ds(rows, 16)] = jnp.concatenate(
                [high.astype(F32), mid.astype(F32), low.astype(F32), jnp.zeros((10, BOT), F32)], axis=0
            ).astype(BF16)
            totals[...] = jnp.zeros_like(totals)

        cols = pl.ds(pl.multiple_of(j * SHARE, SHARE), SHARE)
        block = protos[...].reshape(BOT, SHARE)
        wide = block.astype(F32)
        scale = lax.rsqrt(jnp.sum(wide * wide, axis=0, keepdims=True) + 1e-06)
        unit = (wide * scale).astype(BF16)
        logits = jnp.dot(lhs[...], unit, preferred_element_type=F32)
        current = center[...]
        for v in range(VIEWS):
            each = jnp.exp((logits[v * PADCAP : (v + 1) * PADCAP] - current) / teacher_temp)
            exps[pl.ds(v * PADCAP, PADCAP), cols] = each
            totals[pl.ds(v * PADCAP, PADCAP)] += jnp.broadcast_to(
                jnp.sum(each, axis=1, keepdims=True), (PADCAP, 128)
            )
            summed = logits[rows + v : rows + v + 1] + logits[rows + 2 + v : rows + 3 + v] + logits[rows + 4 + v : rows + 5 + v]
            count = sums[VIEWS + v, 0]
            current = center_momentum * current + (1.0 - center_momentum) * summed / count

        @pl.when(j == z)
        def _():
            new_center[...] = current

    @pl.when(phase == 1)
    def _():
        cols = pl.ds(pl.multiple_of(j * SHARE, SHARE), SHARE)
        slot = lax.broadcasted_iota(jnp.int32, (PADCAP, 1), 0).astype(F32)
        for v in range(VIEWS):
            every = totals[pl.ds(v * PADCAP, PADCAP), pl.ds(0, 1)]
            factor = jnp.where(slot < local[v, 0], PROTO / every, 0.0)
            probs = exps[pl.ds(v * PADCAP, PADCAP), cols] * factor
            out[v] = probs[:CAP].astype(BF16)


def targets_of(normed, sums, local, protos, center):
    full = lambda shape: pl.BlockSpec(shape, lambda p, j: (0,) * len(shape))
    last = NZ - 1
    return pl.pallas_call(
        targets_kernel,
        grid=(2, NZ),
        out_shape=(
            jax.ShapeDtypeStruct((VIEWS, CAP, PROTO), BF16),
            jax.ShapeDtypeStruct((1, SHARE), F32),
        ),
        in_specs=[
            full(normed.shape),
            full(sums.shape),
            full(local.shape),
            pl.BlockSpec((1, 2, NY, 16, SHARE), lambda p, j: (jnp.where(p == 0, j, last), 0, 0, 0, 0)),
            pl.BlockSpec((1, SHARE), lambda p, j: (0, jnp.where(p == 0, j, last))),
        ],
        out_specs=(
            pl.BlockSpec((VIEWS, CAP, SHARE), lambda p, j: (0, 0, p * j)),
            full((1, SHARE)),
        ),
        scratch_shapes=[
            pltpu.VMEM((VIEWS * PADCAP + 16, BOT), BF16),
            pltpu.VMEM((VIEWS * PADCAP, PROTO), F32),
            pltpu.VMEM((VIEWS * PADCAP, 128), F32),
        ],
        compiler_params=pltpu.CompilerParams(vmem_limit_bytes=48 << 20),
        name="targets",
    )(normed, sums, local, protos, center)


def shards(features, patch_mask, w_first, w_second, proto_weight, center):
    w, protos = gather(w_first, w_second, proto_weight)
    normed, part, local = bottleneck(features[:, 0], patch_mask[:, 0], w)
    sums = total(part)
    targets, new_center = targets_of(normed, sums, local, protos, center.reshape(1, PROTO))
    return targets, new_center.reshape(SHARE)


def solution(mesh):
    placed = (
        P(None, ("dp", "head"), None, None),
        P(None, ("dp", "head"), None),
        P("dp", None),
        P("dp", None),
        P("dp", "head"),
        P(),
    )
    return jax.shard_map(
        shards,
        mesh=mesh,
        in_specs=placed,
        out_specs=(P(None, ("dp", "head"), None), P("head")),
        check_vma=False,
    )
```

```python
import functools

import jax
import jax.numpy as jnp
from jax import lax
from jax.experimental import pallas as pl
from jax.experimental.pallas import tpu as pltpu
from jax.sharding import PartitionSpec as P

MESH = pl.DeviceIdType.MESH
HBM = pl.BlockSpec(memory_space=pltpu.MemorySpace.HBM)
VM = pl.BlockSpec(memory_space=pltpu.VMEM)

teacher_temp = 0.04
center_momentum = 0.9

NX, NY, NZ = 4, 8, 8
VIEWS, PATCH, CAP, PADCAP = 2, 196, 98, 104
D, HID, BOT, PROTO = 1024, 2048, 256, 8192
SHARE = PROTO // NZ
ACOLS = 1024
WCOLS = HID + 2 * BOT
ROWS = VIEWS * PADCAP
VMEM_LIMIT = 36 << 20
F32 = jnp.float32
BF16 = jnp.bfloat16


def place():
    dp = lax.axis_index("dp")
    z = lax.axis_index("head")
    return dp // (2 * NY), (dp // 2) % NY, dp % 2, z


def dp_of(x, y, c):
    return (x * NY + y) * 2 + c


Y_ORDER = (0, 1, 7, 2, 6, 3, 5, 4)
RIGHT_HALF = (0, 7, 2, 5)
BY_TIME = {1: 4.2, 7: 4.3, 2: 5.8, 6: 5.9, 3: 7.8, 5: 7.9, 4: 9.8}
STEP = 3.8
MLP_AT = 26.0


def plan():
    events = []
    start = {0: 0.0, 1: 4.4, 3: 4.5, 2: 5.2}
    for d in (1, 3, 2):
        events.append((start[d], "ax", 0, d, 0))
    avail = {0: 0.0, **BY_TIME}
    for d, t in BY_TIME.items():
        events.append((t, "by", 0, d, 0))
    pavail = {0: 4.6}
    for k in range(1, 5):
        pavail[k] = pavail[8 - k] = 4.6 + 3.5 * k
        for side in (0, 1):
            events.append((pavail[k] + 0.01 * side, "py", side, k, 0))
    for k in range(1, 5):
        for side in (0, 1):
            for i, j in enumerate((0, 1, 3, 2)):
                if k == 4 and (j in (0, 1)) != (side == 0):
                    continue
                t = max(start[j] + STEP * k, 4.0 + STEP * (k - 1) + 0.75 * i)
                events.append((t + 0.01 * side, "ay", side, k, j))
    for k in (1, 2):
        for side in (0, 1):
            for i, d in enumerate(Y_ORDER):
                if k == 2 and (d in RIGHT_HALF) != (side == 0):
                    continue
                t = max(avail[d] + STEP, 3.0 + 1.2 * i)
                if k == 2:
                    t = max(t + STEP, 13.0 + 0.6 * i)
                events.append((t + 0.01 * side, "bx", side, k, d))
    whole = {0: pavail[4]}
    for k in range(1, 5):
        for side in (0, 1):
            for i, d in enumerate(Y_ORDER):
                if k == 4 and (d in RIGHT_HALF) != (side == 0):
                    continue
                t = max(pavail[d] + STEP * k, 8.0 + 5.7 * (k - 1) + 0.7 * i)
                events.append((t + 0.01 * side, "pz", side, k, d))
                g = k if side == 0 else 8 - k
                whole[g] = max(whole.get(g, 0.0), t + 0.01 * side)
    events.append((MLP_AT, "mlp", 0, 0, 0))
    sums = [MLP_AT + 2.0 + 5.0 * i for i in (1, 2, 3)]
    for i, t in enumerate(sums):
        events.append((t, "sum", i, 0, 0))
    ready = MLP_AT + 2.0
    for g in sorted(whole, key=whole.get):
        ready = max(ready + 0.7, whole[g] + 2.0)
        events.append((ready, "grp", 0, g, 0))
    return sorted(events)


EVENTS = plan()


def pick_rows(mask, fbuf, rows):
    live = jnp.concatenate([mask[0], mask[1], jnp.zeros((6, PATCH), jnp.int32)], axis=0).astype(F32)
    lanes = VIEWS * PATCH
    at = lax.broadcasted_iota(jnp.int32, (PATCH, lanes), 0)
    to = lax.broadcasted_iota(jnp.int32, (PATCH, lanes), 1)
    mixed = jnp.zeros((1, lanes), F32)
    for v in range(VIEWS):
        spread = (to == 2 * at + v).astype(F32).astype(BF16)
        mixed += jnp.dot(live.astype(BF16), spread, preferred_element_type=F32)[v : v + 1]
    at = lax.broadcasted_iota(jnp.int32, (lanes, lanes), 0)
    to = lax.broadcasted_iota(jnp.int32, (lanes, lanes), 1)
    before = ((at <= to) & ((to - at) % 2 == 0)).astype(F32).astype(BF16)
    mixed8 = jnp.broadcast_to(mixed, (8, lanes))
    rank = jnp.dot(mixed8.astype(BF16), before, preferred_element_type=F32)[0:1]
    row = lax.broadcasted_iota(jnp.int32, (ROWS, lanes), 0)
    lane = lax.broadcasted_iota(jnp.int32, (ROWS, lanes), 1)
    slot = (row // 2 + 1).astype(F32)
    same = (row - lane) % 2 == 0
    pick = ((rank == slot) & same & (mixed > 0.5)).astype(F32).astype(BF16)
    feats = fbuf[...].reshape(lanes, D)
    rows[...] = jnp.dot(pick, feats, preferred_element_type=F32).astype(BF16)
    return [jnp.sum(live[v : v + 1], axis=1, keepdims=True) for v in range(VIEWS)]


def bottleneck(rows, w, normed):
    projected = jnp.zeros((ROWS, BOT), F32)
    wide = HID // NX
    for t in range(NX):
        left = w[:, :, :, :, pl.ds(t * wide, wide)].reshape(D, wide)
        pre = jnp.dot(rows[...], left, preferred_element_type=F32)
        hidden = (0.5 * pre * (1.0 + lax.erf(pre * 0.5**0.5))).astype(BF16)
        low = w[t, :, :, :, pl.ds(HID, BOT)].reshape(16, 16, BOT)
        high = w[t, :, :, :, pl.ds(HID + BOT, BOT)].reshape(16, 16, BOT)
        right = jnp.stack([low, high], axis=1).reshape(wide, BOT)
        projected += jnp.dot(hidden, right, preferred_element_type=F32)
    scale = lax.rsqrt(jnp.sum(projected * projected, axis=-1, keepdims=True) + 1e-06)
    plain = (projected * scale).astype(BF16)
    to = lax.broadcasted_iota(jnp.int32, (BOT, BOT), 1)
    at = lax.broadcasted_iota(jnp.int32, (BOT, BOT), 0)
    source = ((to // 4) % NX) * 64 + ((to // 16) % NY) * 8 + (to // 128) * 4 + to % 4
    ordered = jnp.dot(plain, (at == source).astype(F32).astype(BF16), preferred_element_type=F32)
    normed[...] = ordered.astype(BF16)
    view = lax.broadcasted_iota(jnp.int32, (ROWS, BOT), 0) % 2
    return [jnp.sum(jnp.where(view == v, ordered, 0.0), axis=0, keepdims=True) for v in range(VIEWS)]


def main_kernel(feats, mask_in, w1, w2, pw, center_in, exps, weights, factors, new_center,
                wbuf, pbuf, ubuf, px, fbuf, mask, center, rows, normed, own, land, lsem,
                px_s, px_r, ax_s, ax_r, by_s, by_r, py_s, py_r, ay_s, ay_r, bx_s, bx_r,
                pz_s, pz_r, dd_s, dd_r, ar_s, ar_r):
    x, y, c, z = place()

    def at_x(n):
        return lax.rem(x + n + NX, NX)

    def at_y(n):
        return lax.rem(y + n + NY, NY)

    def at_z(n):
        return lax.rem(z + n + NZ, NZ)

    def dev(nx=0, ny=0, nz=0, other=False):
        return (dp_of(at_x(nx), at_y(ny), 1 - c if other else c), at_z(nz))

    rounds = (
        [dev(nz=n) for n in range(1, 8)],
        [dev(ny=n) for n in range(1, 8)],
        [dev(nx=n % 4, other=n >= 4) for n in range(1, 8)],
    )
    barrier = pltpu.get_barrier_semaphore()
    for peers in rounds:
        for peer in peers:
            pl.semaphore_signal(barrier, inc=1, device_id=peer, device_id_type=MESH)
    cols_a, cols_b = pl.ds(0, ACOLS), pl.ds(ACOLS, WCOLS - ACOLS)
    loads = [
        pltpu.make_async_copy(pw, px.at[x], lsem.at[0]),
        pltpu.make_async_copy(w1, wbuf.at[x, y, c, :, pl.ds(0, HID)], lsem.at[1]),
        pltpu.make_async_copy(w2.at[pl.ds(0, 16)], wbuf.at[x, y, c, :, pl.ds(HID, BOT)], lsem.at[2]),
        pltpu.make_async_copy(w2.at[pl.ds(16, 16)], wbuf.at[x, y, c, :, pl.ds(HID + BOT, BOT)], lsem.at[3]),
        pltpu.make_async_copy(feats, fbuf, lsem.at[4]),
        pltpu.make_async_copy(mask_in, mask, lsem.at[5]),
        pltpu.make_async_copy(center_in, center, lsem.at[6]),
    ]
    for copy in loads:
        copy.start()
    pl.semaphore_wait(barrier, 21)
    for copy in loads[:4]:
        copy.wait()

    sent = []

    def send(ref, s, r, to, dst=None):
        copy = pltpu.make_async_remote_copy(
            src_ref=ref, dst_ref=ref if dst is None else dst, send_sem=s, recv_sem=r, device_id=to, device_id_type=MESH
        )
        copy.start()
        sent.append(copy)

    def landed(ref, s, r, to):
        pltpu.make_async_remote_copy(
            src_ref=ref, dst_ref=ref, send_sem=s, recv_sem=r, device_id=to, device_id_type=MESH
        ).wait_recv()

    def a_ref(nx, ny):
        return wbuf.at[at_x(nx), at_y(ny), c, :, cols_a]

    def b_ref(nx, ny):
        return wbuf.at[at_x(nx), at_y(ny), c, :, cols_b]

    def p_ref(nz, ny, side=None):
        cols = pl.ds(0, SHARE) if side is None else pl.ds(side * (SHARE // 2), SHARE // 2)
        return pbuf.at[at_z(nz), c, at_y(ny), :, cols]

    def sgn(side):
        return 1 if side == 0 else -1

    def back(side, k):
        return -k * sgn(side)

    counts = {("p", 0): 9, ("p4"): 2}
    for g in range(NY):
        counts["a", g] = 4
        counts.setdefault(("p", g), 8)
    for g in range(NX):
        counts["b", g] = 8

    def done(kind, g):
        counts[kind, g] -= 1
        if counts[kind, g]:
            return
        to = dev(other=True)
        if kind == "a":
            send(wbuf.at[:, at_y(-g), c, :, cols_a], dd_s.at[g], dd_r.at[g], to)
        elif kind == "b":
            send(wbuf.at[at_x(-g), :, c, :, cols_b], dd_s.at[8 + g], dd_r.at[8 + g], to)
        else:
            send(pbuf.at[at_z(-g), c], dd_s.at[12 + g], dd_r.at[12 + g], to)

    def forward_py(side, k):
        ref = p_ref(0, back(side, k - 1), None if k <= 3 else side)
        send(ref, py_s.at[side, k - 1], py_r.at[side, k - 1], dev(ny=sgn(side)))

    def forward_ay(side, k, j):
        if k == 4 and (j in (0, 1)) != (side == 0):
            return
        send(a_ref(-j, back(side, k - 1)), ay_s.at[side, k - 1, j], ay_r.at[side, k - 1, j], dev(ny=sgn(side)))

    def forward_bx(side, k, d):
        if k == 2 and (d in RIGHT_HALF) != (side == 0):
            return
        send(b_ref(back(side, k - 1), -d), bx_s.at[side, k - 1, d], bx_r.at[side, k - 1, d], dev(nx=sgn(side)))

    def forward_pz(side, k, d):
        if k == 4 and (d in RIGHT_HALF) != (side == 0):
            return
        send(p_ref(back(side, k - 1), -d), pz_s.at[side, k - 1, d], pz_r.at[side, k - 1, d], dev(nz=sgn(side)))

    def sum_round(i):
        for n, peer in enumerate(rounds[i]):
            send(own.at[i], ar_s.at[i, n], ar_r.at[i, n], peer, land.at[i, n])

    for n in (1, 3, 2):
        send(px.at[x], px_s.at[n], px_r.at[n], dev(nx=n))
    for n in (1, 3, 2):
        send(a_ref(0, 0), ax_s.at[n], ax_r.at[n], dev(nx=n))
    for n in (1, 7, 2, 6, 3, 5, 4):
        send(b_ref(0, 0), by_s.at[n], by_r.at[n], dev(ny=n))
    for side in (0, 1):
        forward_bx(side, 1, 0)
        forward_ay(side, 1, 0)
    done("a", 0)
    done("b", 0)

    for copy in loads[4:]:
        copy.wait()
    local = pick_rows(mask, fbuf, rows)

    for n in (1, 3, 2):
        landed(px.at[at_x(-n)], px_s.at[n], px_r.at[n], dev(nx=n))
    pbuf[z, c, y] = px[...].reshape(16, SHARE)
    other = 1 - c

    def handle(event):
        _, kind, side, k, j = event
        if kind == "ax":
            landed(a_ref(-k, 0), ax_s.at[k], ax_r.at[k], dev(nx=k))
            for s in (0, 1):
                forward_ay(s, 1, k)
            done("a", 0)
        elif kind == "by":
            landed(b_ref(0, -k), by_s.at[k], by_r.at[k], dev(ny=k))
            for s in (0, 1):
                forward_bx(s, 1, k)
            done("b", 0)
        elif kind == "py":
            ref = p_ref(0, back(side, k), None if k < 4 else side)
            landed(ref, py_s.at[side, k - 1], py_r.at[side, k - 1], dev(ny=1))
            if k < 4:
                forward_py(side, k + 1)
            else:
                counts["p4"] -= 1
            if k < 4 or counts["p4"] == 0:
                for s in (0, 1):
                    forward_pz(s, 1, k if side == 0 else 8 - k)
            done("p", 0)
        elif kind == "ay":
            landed(a_ref(-j, back(side, k)), ay_s.at[side, k - 1, j], ay_r.at[side, k - 1, j], dev(ny=1))
            if k < 4:
                forward_ay(side, k + 1, j)
            done("a", k if side == 0 else 8 - k)
        elif kind == "bx":
            landed(b_ref(back(side, k), -j), bx_s.at[side, k - 1, j], bx_r.at[side, k - 1, j], dev(nx=1))
            if k < 2:
                forward_bx(side, k + 1, j)
            done("b", k if side == 0 else 4 - k)
        elif kind == "pz":
            landed(p_ref(back(side, k), -j), pz_s.at[side, k - 1, j], pz_r.at[side, k - 1, j], dev(nz=1))
            if k < 4:
                forward_pz(side, k + 1, j)
            done("p", k if side == 0 else 8 - k)
        elif kind == "mlp":
            for g in range(8):
                landed(wbuf.at[:, at_y(-g), other, :, cols_a], dd_s.at[g], dd_r.at[g], dev(other=True))
            for g in range(4):
                landed(wbuf.at[at_x(-g), :, other, :, cols_b], dd_s.at[8 + g], dd_r.at[8 + g], dev(other=True))
            sums = bottleneck(rows, wbuf, normed)
            own[0] = jnp.concatenate(sums + [jnp.broadcast_to(n, (1, BOT)) for n in local], axis=0)
            sum_round(0)
        elif kind == "sum":
            total = own[side]
            for n, peer in enumerate(rounds[side]):
                landed(land.at[side, n], ar_s.at[side, n], ar_r.at[side, n], peer)
                total = total + land[side, n]
            own[side + 1] = total
            if side < 2:
                sum_round(side + 1)
        else:
            at = at_z(-k)
            landed(pbuf.at[at, other], dd_s.at[12 + k], dd_r.at[12 + k], dev(other=True))
            wide = pbuf[at].reshape(BOT, SHARE).astype(F32)
            scale = lax.rsqrt(jnp.sum(wide * wide, axis=0, keepdims=True) + 1e-06)
            unit = (wide * scale).astype(BF16)
            ubuf[at] = unit
            logits = jnp.dot(normed[...], unit, preferred_element_type=F32)
            exps[:, pl.ds(pl.multiple_of(at * SHARE, SHARE), SHARE)] = jnp.exp(logits / teacher_temp)

    early = [e for e in EVENTS if e[1] in ("ax", "by") and e[0] < 4.55]
    for event in early:
        handle(event)
    for side in (0, 1):
        forward_py(side, 1)
        forward_pz(side, 1, 0)
    done("p", 0)
    for event in EVENTS:
        if event not in early:
            handle(event)
    assert not any(v for k, v in counts.items()), counts

    whole = own[3]
    high = whole[:VIEWS].astype(BF16).astype(F32)
    mid = (whole[:VIEWS] - high).astype(BF16).astype(F32)
    low = whole[:VIEWS] - high - mid
    parts = jnp.concatenate([high, mid, low, jnp.zeros((10, BOT), F32)], axis=0).astype(BF16)
    acc = jnp.zeros((ROWS, 128), F32)
    parity = lax.broadcasted_iota(jnp.int32, (8, SHARE), 0) % 2
    for at in range(NZ):
        cols = pl.ds(at * SHARE, SHARE)
        split = jnp.dot(parts, ubuf[at], preferred_element_type=F32)
        current, pair = center[:, cols], []
        for v in range(VIEWS):
            pair.append(jnp.exp(current / -teacher_temp))
            summed = split[v : v + 1] + split[2 + v : 3 + v] + split[4 + v : 5 + v]
            current = center_momentum * current + (1.0 - center_momentum) * summed / whole[VIEWS + v : VIEWS + v + 1, 0:1]
        pattern = jnp.where(parity == 0, pair[0], pair[1])
        weights[:, cols] = pattern
        shares = exps[:, cols].reshape(ROWS // 8, 8, SHARE) * pattern[None]
        shares = shares.reshape(ROWS, SHARE)
        for i in range(SHARE // 128):
            acc += shares[:, i * 128 : (i + 1) * 128]

        @pl.when(z == at)
        def _(current=current):
            new_center[...] = current

    row = lax.broadcasted_iota(jnp.int32, (ROWS, 1), 0)
    filled = jnp.where(row % 2 == 0, local[0], local[1]) > (row // 2).astype(F32)
    factor = jnp.where(filled, PROTO / jnp.sum(acc, axis=1, keepdims=True), 0.0)
    factors[...] = jnp.broadcast_to(factor, (ROWS, 128))
    for copy in sent:
        copy.wait_send()


def main_part(feats, patch_mask, w_first, w_second, proto_weight, center):
    dma = pltpu.SemaphoreType.DMA
    return pl.pallas_call(
        main_kernel,
        out_shape=(
            jax.ShapeDtypeStruct((ROWS, PROTO), F32),
            jax.ShapeDtypeStruct((8, PROTO), F32),
            jax.ShapeDtypeStruct((ROWS, 128), F32),
            jax.ShapeDtypeStruct((1, SHARE), F32),
        ),
        in_specs=[HBM] * 6,
        out_specs=(VM,) * 4,
        scratch_shapes=[
            pltpu.VMEM((NX, NY, 2, 16, WCOLS), BF16),
            pltpu.VMEM((NZ, 2, NY, 16, SHARE), BF16),
            pltpu.VMEM((NZ, BOT, SHARE), BF16),
            pltpu.VMEM((NX, 4, SHARE), BF16),
            pltpu.VMEM((PATCH, VIEWS, D), BF16),
            pltpu.VMEM((VIEWS, 1, PATCH), jnp.int32),
            pltpu.VMEM((1, PROTO), F32),
            pltpu.VMEM((ROWS, D), BF16),
            pltpu.VMEM((ROWS, BOT), BF16),
            pltpu.VMEM((4, 2 * VIEWS, BOT), F32),
            pltpu.VMEM((3, 7, 2 * VIEWS, BOT), F32),
            dma((7,)),
            dma((4,)), dma((4,)), dma((4,)), dma((4,)),
            dma((8,)), dma((8,)), dma((2, 4)), dma((2, 4)),
            dma((2, 4, 4)), dma((2, 4, 4)), dma((2, 2, 8)), dma((2, 2, 8)),
            dma((2, 4, 8)), dma((2, 4, 8)), dma((20,)), dma((20,)),
            dma((3, 7)), dma((3, 7)),
        ],
        compiler_params=pltpu.CompilerParams(
            collective_id=0, has_side_effects=True, vmem_limit_bytes=VMEM_LIMIT
        ),
        name="main_part",
    )(feats, patch_mask, w_first, w_second, proto_weight, center)


def write_kernel(exps, weights, factors, center, out, center_out):
    center_out[...] = center[...]
    for r in range(0, ROWS, 16):
        keep = min(16, VIEWS * CAP - r) // 2
        probs = []
        for h in (r, r + 8):
            probs.append(exps[pl.ds(h, 8)] * weights[...] * factors[pl.ds(h, 8), pl.ds(0, 1)])
        block = jnp.concatenate(probs, axis=0).astype(BF16)
        if keep > 0:
            out[pl.ds(r // 2, keep)] = block.reshape(8, VIEWS, block.shape[1])[:keep]


def write(exps, weights, factors, new_center):
    wide = 1024
    return pl.pallas_call(
        write_kernel,
        grid=(PROTO // wide,),
        out_shape=(
            jax.ShapeDtypeStruct((CAP, VIEWS, PROTO), BF16),
            jax.ShapeDtypeStruct((1, SHARE), F32),
        ),
        in_specs=[
            pl.BlockSpec((ROWS, wide), lambda j: (0, j)),
            pl.BlockSpec((8, wide), lambda j: (0, j)),
            pl.BlockSpec((ROWS, 128), lambda j: (0, 0)),
            pl.BlockSpec((1, SHARE), lambda j: (0, 0)),
        ],
        out_specs=(
            pl.BlockSpec((CAP, VIEWS, wide), lambda j: (0, 0, j)),
            pl.BlockSpec((1, SHARE), lambda j: (0, 0)),
        ),
        compiler_params=pltpu.CompilerParams(vmem_limit_bytes=16 << 20),
        name="write",
    )(exps, weights, factors, new_center)


def shards(features, patch_mask, w_first, w_second, proto_weight, center):
    feats = features[:, 0].transpose(1, 0, 2)
    inputs = (feats, patch_mask, w_first, w_second, proto_weight, center.reshape(1, PROTO))
    inputs = [pltpu.with_memory_space_constraint(a, pltpu.MemorySpace.HBM) for a in inputs]
    exps, weights, factors, new_center = main_part(*inputs)
    targets, new_center = write(exps, weights, factors, new_center)
    return targets.transpose(1, 0, 2), new_center.reshape(SHARE)


def solution(mesh):
    placed = (
        P(None, ("dp", "head"), None, None),
        P(None, ("dp", "head"), None),
        P("dp", None),
        P("dp", None),
        P("dp", "head"),
        P(),
    )
    return jax.shard_map(
        shards,
        mesh=mesh,
        in_specs=placed,
        out_specs=(P(None, ("dp", "head"), None), P("head")),
        check_vma=False,
    )
```

```python
import functools

import jax
import jax.numpy as jnp
from jax import lax
from jax.experimental import pallas as pl
from jax.experimental.pallas import tpu as pltpu
from jax.sharding import PartitionSpec as P

MESH = pl.DeviceIdType.MESH
HBM = pl.BlockSpec(memory_space=pltpu.MemorySpace.HBM)
VM = pl.BlockSpec(memory_space=pltpu.VMEM)

teacher_temp = 0.04
center_momentum = 0.9

NX, NY, NZ = 4, 8, 8
VIEWS, PATCH, CAP, PADCAP = 2, 196, 98, 104
D, HID, BOT, PROTO = 1024, 2048, 256, 8192
SHARE = PROTO // NZ
ACOLS = 1024
WCOLS = HID + 2 * BOT
ROWS = VIEWS * PADCAP
VMEM_LIMIT = 36 << 20
F32 = jnp.float32
BF16 = jnp.bfloat16


def place():
    dp = lax.axis_index("dp")
    z = lax.axis_index("head")
    return dp // (2 * NY), (dp // 2) % NY, dp % 2, z


def dp_of(x, y, c):
    return (x * NY + y) * 2 + c


Y_ORDER = (0, 1, 7, 2, 6, 3, 5, 4)
RIGHT_HALF = (0, 7, 2, 5)
BY_TIME = {1: 4.2, 7: 4.3, 2: 5.5, 6: 5.6, 3: 9.5, 5: 9.6, 4: 10.5}
PX_TIME = {0: 6.5, 1: 11.5, 3: 11.6, 2: 12.6}
STEP = 3.8
MLP_AT = 24.0


def plan():
    events = []
    start = {0: 0.0, 1: 4.4, 3: 4.5, 2: 5.2}
    for d in (1, 3, 2):
        events.append((start[d], "ax", 0, d, 0))
    avail = {0: 0.0, **BY_TIME}
    for d, t in BY_TIME.items():
        events.append((t, "by", 0, d, 0))
    events.append((BY_TIME[4] + 0.1, "by", 1, 4, 0))
    events.append((PX_TIME[0], "pack", 0, 0, 0))
    for d in (1, 3, 2):
        events.append((PX_TIME[d], "px", 0, d, 0))
    for k in range(1, 5):
        for side in (0, 1):
            for i, j in enumerate((0, 1, 3, 2)):
                if k == 4 and (j in (0, 1)) != (side == 0):
                    continue
                t = max(start[j] + STEP * k, 4.0 + STEP * (k - 1) + 0.75 * i)
                events.append((t + 0.01 * side, "ay", side, k, j))
    for k in (1, 2):
        for side in (0, 1):
            for i, d in enumerate(Y_ORDER):
                if k == 2 and (d in RIGHT_HALF) != (side == 0):
                    continue
                t = max(avail[d] + STEP, 3.0 + 1.2 * i)
                if k == 2:
                    t = max(t + STEP, 13.0 + 0.6 * i)
                events.append((t + 0.01 * side, "bx", side, k, d))
    whole = {0: PX_TIME[2]}
    for k in range(1, 5):
        for side in (0, 1):
            for i, d in enumerate((0, 1, 3, 2)):
                for h in (0, 1):
                    if k == 4 and h != side:
                        continue
                    t = max(PX_TIME[d] + STEP * k + 0.7 * h, 8.5 + 5.7 * (k - 1) + 1.4 * i + 0.7 * h)
                    events.append((t + 0.01 * side, "pz", side, k, 2 * d + h))
                    g = k if side == 0 else 8 - k
                    whole[g] = max(whole.get(g, 0.0), t + 0.01 * side)
    events.append((MLP_AT, "mlp", 0, 0, 0))
    for i in range(3):
        events.append((MLP_AT + 2.0 + 4.5 * (i + 1), "sum", i, 0, 0))
    ready = MLP_AT + 2.0
    for g in sorted(whole, key=whole.get):
        ready = max(ready + 0.7, whole[g] + 2.0)
        events.append((ready, "grp", 0, g, 0))
    return sorted(events)


EVENTS = plan()


def pick_rows(mask, fbuf, rows):
    live = jnp.concatenate([mask[0], mask[1], jnp.zeros((6, PATCH), jnp.int32)], axis=0).astype(F32)
    lanes = VIEWS * PATCH
    at = lax.broadcasted_iota(jnp.int32, (PATCH, lanes), 0)
    to = lax.broadcasted_iota(jnp.int32, (PATCH, lanes), 1)
    mixed = jnp.zeros((1, lanes), F32)
    for v in range(VIEWS):
        spread = (to == 2 * at + v).astype(F32).astype(BF16)
        mixed += jnp.dot(live.astype(BF16), spread, preferred_element_type=F32)[v : v + 1]
    at = lax.broadcasted_iota(jnp.int32, (lanes, lanes), 0)
    to = lax.broadcasted_iota(jnp.int32, (lanes, lanes), 1)
    before = ((at <= to) & ((to - at) % 2 == 0)).astype(F32).astype(BF16)
    mixed8 = jnp.broadcast_to(mixed, (8, lanes))
    rank = jnp.dot(mixed8.astype(BF16), before, preferred_element_type=F32)[0:1]
    row = lax.broadcasted_iota(jnp.int32, (ROWS, lanes), 0)
    lane = lax.broadcasted_iota(jnp.int32, (ROWS, lanes), 1)
    slot = (row // 2 + 1).astype(F32)
    same = (row - lane) % 2 == 0
    pick = ((rank == slot) & same & (mixed > 0.5)).astype(F32).astype(BF16)
    feats = fbuf[...].reshape(lanes, D)
    rows[...] = jnp.dot(pick, feats, preferred_element_type=F32).astype(BF16)
    return [jnp.sum(live[v : v + 1], axis=1, keepdims=True) for v in range(VIEWS)]


def bottleneck(rows, w, normed):
    projected = jnp.zeros((ROWS, BOT), F32)
    wide = HID // NX
    for t in range(NX):
        left = w[:, :, :, :, pl.ds(t * wide, wide)].reshape(D, wide)
        pre = jnp.dot(rows[...], left, preferred_element_type=F32)
        hidden = (0.5 * pre * (1.0 + lax.erf(pre * 0.5**0.5))).astype(BF16)
        low = w[t, :, :, :, pl.ds(HID, BOT)].reshape(16, 16, BOT)
        high = w[t, :, :, :, pl.ds(HID + BOT, BOT)].reshape(16, 16, BOT)
        right = jnp.stack([low, high], axis=1).reshape(wide, BOT)
        projected += jnp.dot(hidden, right, preferred_element_type=F32)
    scale = lax.rsqrt(jnp.sum(projected * projected, axis=-1, keepdims=True) + 1e-06)
    plain = (projected * scale).astype(BF16)
    to = lax.broadcasted_iota(jnp.int32, (BOT, BOT), 1)
    at = lax.broadcasted_iota(jnp.int32, (BOT, BOT), 0)
    source = ((to // 32) % NX) * 64 + ((to // 4) % NY) * 8 + (to // 128) * 4 + to % 4
    ordered = jnp.dot(plain, (at == source).astype(F32).astype(BF16), preferred_element_type=F32)
    normed[...] = ordered.astype(BF16)
    view = lax.broadcasted_iota(jnp.int32, (ROWS, BOT), 0) % 2
    return [jnp.sum(jnp.where(view == v, ordered, 0.0), axis=0, keepdims=True) for v in range(VIEWS)]


def main_kernel(feats, mask_in, w1, w2, pw, center_in, exps, weights, factors, new_center,
                wbuf, pbuf, ubuf, stage, fbuf, mask, center, rows, normed, own, land, lsem,
                px_s, px_r, ax_s, ax_r, by_s, by_r, py_s, py_r, ay_s, ay_r, bx_s, bx_r,
                pz_s, pz_r, dd_s, dd_r, ar_s, ar_r):
    x, y, c, z = place()

    def at_x(n):
        return lax.rem(x + n + NX, NX)

    def at_y(n):
        return lax.rem(y + n + NY, NY)

    def at_z(n):
        return lax.rem(z + n + NZ, NZ)

    def dev(nx=0, ny=0, nz=0, other=False):
        return (dp_of(at_x(nx), at_y(ny), 1 - c if other else c), at_z(nz))

    rounds = (
        [dev(nz=n) for n in range(1, 8)],
        [dev(ny=n) for n in range(1, 8)],
        [dev(nx=n % 4, other=n >= 4) for n in range(1, 8)],
    )
    barrier = pltpu.get_barrier_semaphore()
    for peers in rounds:
        for peer in peers:
            pl.semaphore_signal(barrier, inc=1, device_id=peer, device_id_type=MESH)
    cols_a, cols_b = pl.ds(0, ACOLS), pl.ds(ACOLS, WCOLS - ACOLS)
    loads = [
        pltpu.make_async_copy(pw, stage.at[y], lsem.at[0]),
        pltpu.make_async_copy(w1, wbuf.at[x, y, c, :, pl.ds(0, HID)], lsem.at[1]),
        pltpu.make_async_copy(w2.at[pl.ds(0, 16)], wbuf.at[x, y, c, :, pl.ds(HID, BOT)], lsem.at[2]),
        pltpu.make_async_copy(w2.at[pl.ds(16, 16)], wbuf.at[x, y, c, :, pl.ds(HID + BOT, BOT)], lsem.at[3]),
        pltpu.make_async_copy(feats, fbuf, lsem.at[4]),
        pltpu.make_async_copy(mask_in, mask, lsem.at[5]),
        pltpu.make_async_copy(center_in, center, lsem.at[6]),
    ]
    for copy in loads:
        copy.start()
    pl.semaphore_wait(barrier, 21)
    for copy in loads[:4]:
        copy.wait()

    sent = []

    def send(ref, s, r, to, dst=None):
        copy = pltpu.make_async_remote_copy(
            src_ref=ref, dst_ref=ref if dst is None else dst, send_sem=s, recv_sem=r, device_id=to, device_id_type=MESH
        )
        copy.start()
        sent.append(copy)

    def landed(ref, s, r, to):
        pltpu.make_async_remote_copy(
            src_ref=ref, dst_ref=ref, send_sem=s, recv_sem=r, device_id=to, device_id_type=MESH
        ).wait_recv()

    def a_ref(nx, ny):
        return wbuf.at[at_x(nx), at_y(ny), c, :, cols_a]

    def b_ref(nx, ny, side=None):
        wide = WCOLS - ACOLS
        cols = cols_b if side is None else pl.ds(ACOLS + side * (wide // 2), wide // 2)
        return wbuf.at[at_x(nx), at_y(ny), c, :, cols]

    def p_ref(nz, nx, half=None):
        part = pl.ds(0, 4 * NY) if half is None else pl.ds(half * 2 * NY, 2 * NY)
        return pbuf.at[at_z(nz), c, at_x(nx), part]

    def sgn(side):
        return 1 if side == 0 else -1

    def back(side, k):
        return -k * sgn(side)

    counts = {("p", 0): 4, ("b", 0): 9, "far": 2}
    for g in range(NY):
        counts["a", g] = 4
        counts.setdefault(("p", g), 8)
    for g in range(NX):
        counts.setdefault(("b", g), 8)

    def done(kind, g):
        counts[kind, g] -= 1
        if counts[kind, g]:
            return
        to = dev(other=True)
        if kind == "a":
            send(wbuf.at[:, at_y(-g), c, :, cols_a], dd_s.at[g], dd_r.at[g], to)
        elif kind == "b":
            send(wbuf.at[at_x(-g), :, c, :, cols_b], dd_s.at[8 + g], dd_r.at[8 + g], to)
        else:
            send(pbuf.at[at_z(-g), c], dd_s.at[12 + g], dd_r.at[12 + g], to)

    def forward_ay(side, k, j):
        if k == 4 and (j in (0, 1)) != (side == 0):
            return
        send(a_ref(-j, back(side, k - 1)), ay_s.at[side, k - 1, j], ay_r.at[side, k - 1, j], dev(ny=sgn(side)))

    def forward_bx(side, k, d):
        if k == 2 and (d in RIGHT_HALF) != (side == 0):
            return
        send(b_ref(back(side, k - 1), -d), bx_s.at[side, k - 1, d], bx_r.at[side, k - 1, d], dev(nx=sgn(side)))

    def forward_pz(side, k, j):
        if k == 4 and j % 2 != side:
            return
        send(p_ref(back(side, k - 1), -(j // 2), j % 2), pz_s.at[side, k - 1, j], pz_r.at[side, k - 1, j], dev(nz=sgn(side)))

    def sum_round(i):
        for n, peer in enumerate(rounds[i]):
            send(own.at[i], ar_s.at[i, n], ar_r.at[i, n], peer, land.at[i, n])

    for n in (4, 3, 5, 2, 6, 1, 7):
        send(stage.at[y], py_s.at[n], py_r.at[n], dev(ny=n))
    for n in (1, 3, 2):
        send(a_ref(0, 0), ax_s.at[n], ax_r.at[n], dev(nx=n))
    for n in (1, 7, 2, 6):
        send(b_ref(0, 0), by_s.at[n], by_r.at[n], dev(ny=n))
    for side in (0, 1):
        forward_bx(side, 1, 0)
        forward_ay(side, 1, 0)
    done("a", 0)
    done("b", 0)

    for copy in loads[4:]:
        copy.wait()
    local = pick_rows(mask, fbuf, rows)

    other = 1 - c

    def handle(event):
        _, kind, side, k, j = event
        if kind == "ax":
            landed(a_ref(-k, 0), ax_s.at[k], ax_r.at[k], dev(nx=k))
            for s in (0, 1):
                forward_ay(s, 1, k)
            done("a", 0)
        elif kind == "by":
            slot = 8 if side else k
            landed(b_ref(0, -k, side if k == 4 else None), by_s.at[slot], by_r.at[slot], dev(ny=k))
            if k in (2, 6):
                way = 1 if k == 2 else -1
                near, far, half = (3, 4, 0) if k == 2 else (5, 8, 1)
                send(b_ref(0, -k), by_s.at[near], by_r.at[near], dev(ny=way))
                send(b_ref(0, -k, half), by_s.at[far], by_r.at[far], dev(ny=2 * way))
            if k == 4:
                counts["far"] -= 1
            if k != 4 or counts["far"] == 0:
                for s in (0, 1):
                    forward_bx(s, 1, k)
            done("b", 0)
        elif kind == "pack":
            for n in range(1, NY):
                landed(stage.at[at_y(-n)], py_s.at[n], py_r.at[n], dev(ny=n))
            pbuf[z, c, x] = stage[...].reshape(4 * NY, SHARE)
            for n in (1, 3, 2):
                send(p_ref(0, 0), px_s.at[n], px_r.at[n], dev(nx=n))
            for j in (0, 1):
                for s in (0, 1):
                    forward_pz(s, 1, j)
            done("p", 0)
        elif kind == "px":
            landed(p_ref(0, -k), px_s.at[k], px_r.at[k], dev(nx=k))
            for j in (2 * k, 2 * k + 1):
                for s in (0, 1):
                    forward_pz(s, 1, j)
            done("p", 0)
        elif kind == "ay":
            landed(a_ref(-j, back(side, k)), ay_s.at[side, k - 1, j], ay_r.at[side, k - 1, j], dev(ny=1))
            if k < 4:
                forward_ay(side, k + 1, j)
            done("a", k if side == 0 else 8 - k)
        elif kind == "bx":
            landed(b_ref(back(side, k), -j), bx_s.at[side, k - 1, j], bx_r.at[side, k - 1, j], dev(nx=1))
            if k < 2:
                forward_bx(side, k + 1, j)
            done("b", k if side == 0 else 4 - k)
        elif kind == "pz":
            landed(p_ref(back(side, k), -(j // 2), j % 2), pz_s.at[side, k - 1, j], pz_r.at[side, k - 1, j], dev(nz=1))
            if k < 4:
                forward_pz(side, k + 1, j)
            done("p", k if side == 0 else 8 - k)
        elif kind == "mlp":
            for g in range(8):
                landed(wbuf.at[:, at_y(-g), other, :, cols_a], dd_s.at[g], dd_r.at[g], dev(other=True))
            for g in range(4):
                landed(wbuf.at[at_x(-g), :, other, :, cols_b], dd_s.at[8 + g], dd_r.at[8 + g], dev(other=True))
            sums = bottleneck(rows, wbuf, normed)
            own[0] = jnp.concatenate(sums + [jnp.broadcast_to(n, (1, BOT)) for n in local], axis=0)
            sum_round(0)
        elif kind == "sum":
            total = own[side]
            for n, peer in enumerate(rounds[side]):
                landed(land.at[side, n], ar_s.at[side, n], ar_r.at[side, n], peer)
                total = total + land[side, n]
            own[side + 1] = total
            if side < 2:
                sum_round(side + 1)
        else:
            at = at_z(-k)
            landed(pbuf.at[at, other], dd_s.at[12 + k], dd_r.at[12 + k], dev(other=True))
            wide = pbuf[at].reshape(BOT, SHARE).astype(F32)
            scale = lax.rsqrt(jnp.sum(wide * wide, axis=0, keepdims=True) + 1e-06)
            unit = (wide * scale).astype(BF16)
            ubuf[at] = unit
            logits = jnp.dot(normed[...], unit, preferred_element_type=F32)
            exps[:, pl.ds(pl.multiple_of(at * SHARE, SHARE), SHARE)] = jnp.exp(logits / teacher_temp)

    for event in EVENTS:
        handle(event)
    assert not any(v for k, v in counts.items()), counts

    whole = own[3]
    high = whole[:VIEWS].astype(BF16).astype(F32)
    mid = (whole[:VIEWS] - high).astype(BF16).astype(F32)
    low = whole[:VIEWS] - high - mid
    parts = jnp.concatenate([high, mid, low, jnp.zeros((10, BOT), F32)], axis=0).astype(BF16)
    acc = jnp.zeros((ROWS, 128), F32)
    parity = lax.broadcasted_iota(jnp.int32, (8, SHARE), 0) % 2
    for at in range(NZ):
        cols = pl.ds(at * SHARE, SHARE)
        split = jnp.dot(parts, ubuf[at], preferred_element_type=F32)
        current, pair = center[:, cols], []
        for v in range(VIEWS):
            pair.append(jnp.exp(current / -teacher_temp))
            summed = split[v : v + 1] + split[2 + v : 3 + v] + split[4 + v : 5 + v]
            current = center_momentum * current + (1.0 - center_momentum) * summed / whole[VIEWS + v : VIEWS + v + 1, 0:1]
        pattern = jnp.where(parity == 0, pair[0], pair[1])
        weights[:, cols] = pattern
        shares = exps[:, cols].reshape(ROWS // 8, 8, SHARE) * pattern[None]
        shares = shares.reshape(ROWS, SHARE)
        for i in range(SHARE // 128):
            acc += shares[:, i * 128 : (i + 1) * 128]

        @pl.when(z == at)
        def _(current=current):
            new_center[...] = current

    row = lax.broadcasted_iota(jnp.int32, (ROWS, 1), 0)
    filled = jnp.where(row % 2 == 0, local[0], local[1]) > (row // 2).astype(F32)
    factor = jnp.where(filled, PROTO / jnp.sum(acc, axis=1, keepdims=True), 0.0)
    factors[...] = jnp.broadcast_to(factor, (ROWS, 128))
    for copy in sent:
        copy.wait_send()


def main_part(feats, patch_mask, w_first, w_second, proto_weight, center):
    dma = pltpu.SemaphoreType.DMA
    return pl.pallas_call(
        main_kernel,
        out_shape=(
            jax.ShapeDtypeStruct((ROWS, PROTO), F32),
            jax.ShapeDtypeStruct((8, PROTO), F32),
            jax.ShapeDtypeStruct((ROWS, 128), F32),
            jax.ShapeDtypeStruct((1, SHARE), F32),
        ),
        in_specs=[HBM] * 6,
        out_specs=(VM,) * 4,
        scratch_shapes=[
            pltpu.VMEM((NX, NY, 2, 16, WCOLS), BF16),
            pltpu.VMEM((NZ, 2, NX, 4 * NY, SHARE), BF16),
            pltpu.VMEM((NZ, BOT, SHARE), BF16),
            pltpu.VMEM((NY, 4, SHARE), BF16),
            pltpu.VMEM((PATCH, VIEWS, D), BF16),
            pltpu.VMEM((VIEWS, 1, PATCH), jnp.int32),
            pltpu.VMEM((1, PROTO), F32),
            pltpu.VMEM((ROWS, D), BF16),
            pltpu.VMEM((ROWS, BOT), BF16),
            pltpu.VMEM((4, 2 * VIEWS, BOT), F32),
            pltpu.VMEM((3, 7, 2 * VIEWS, BOT), F32),
            dma((7,)),
            dma((4,)), dma((4,)), dma((4,)), dma((4,)),
            dma((9,)), dma((9,)), dma((8,)), dma((8,)),
            dma((2, 4, 4)), dma((2, 4, 4)), dma((2, 2, 8)), dma((2, 2, 8)),
            dma((2, 4, 8)), dma((2, 4, 8)), dma((20,)), dma((20,)),
            dma((3, 7)), dma((3, 7)),
        ],
        compiler_params=pltpu.CompilerParams(
            collective_id=0, has_side_effects=True, vmem_limit_bytes=VMEM_LIMIT
        ),
        name="main_part",
    )(feats, patch_mask, w_first, w_second, proto_weight, center)


def write_kernel(exps, weights, factors, center, out, center_out):
    center_out[...] = center[...]
    for r in range(0, ROWS, 16):
        keep = min(16, VIEWS * CAP - r) // 2
        probs = []
        for h in (r, r + 8):
            probs.append(exps[pl.ds(h, 8)] * weights[...] * factors[pl.ds(h, 8), pl.ds(0, 1)])
        block = jnp.concatenate(probs, axis=0).astype(BF16)
        if keep > 0:
            out[pl.ds(r // 2, keep)] = block.reshape(8, VIEWS, block.shape[1])[:keep]


def write(exps, weights, factors, new_center):
    wide = 1024
    return pl.pallas_call(
        write_kernel,
        grid=(PROTO // wide,),
        out_shape=(
            jax.ShapeDtypeStruct((CAP, VIEWS, PROTO), BF16),
            jax.ShapeDtypeStruct((1, SHARE), F32),
        ),
        in_specs=[
            pl.BlockSpec((ROWS, wide), lambda j: (0, j)),
            pl.BlockSpec((8, wide), lambda j: (0, j)),
            pl.BlockSpec((ROWS, 128), lambda j: (0, 0)),
            pl.BlockSpec((1, SHARE), lambda j: (0, 0)),
        ],
        out_specs=(
            pl.BlockSpec((CAP, VIEWS, wide), lambda j: (0, 0, j)),
            pl.BlockSpec((1, SHARE), lambda j: (0, 0)),
        ),
        compiler_params=pltpu.CompilerParams(vmem_limit_bytes=16 << 20),
        name="write",
    )(exps, weights, factors, new_center)


def shards(features, patch_mask, w_first, w_second, proto_weight, center):
    feats = features[:, 0].transpose(1, 0, 2)
    inputs = (feats, patch_mask, w_first, w_second, proto_weight, center.reshape(1, PROTO))
    inputs = [pltpu.with_memory_space_constraint(a, pltpu.MemorySpace.HBM) for a in inputs]
    exps, weights, factors, new_center = main_part(*inputs)
    targets, new_center = write(exps, weights, factors, new_center)
    return targets.transpose(1, 0, 2), new_center.reshape(SHARE)


def solution(mesh):
    placed = (
        P(None, ("dp", "head"), None, None),
        P(None, ("dp", "head"), None),
        P("dp", None),
        P("dp", None),
        P("dp", "head"),
        P(),
    )
    return jax.shard_map(
        shards,
        mesh=mesh,
        in_specs=placed,
        out_specs=(P(None, ("dp", "head"), None), P("head")),
        check_vma=False,
    )
```
